32 devices in a mesh: grid: 4 (over y, x), fsdp: 8 (over z, core).
Axes of the slice: x: 2, y: 2, z: 4, core: 2. Of those that a mesh axis runs over, the one named last changes fastest.
Arguments:
- hidden: bfloat16 [512, 4096], P('fsdp'), may hold values from -16 to 16
- norm_gain: float32 [4096], replicated, may hold values from 0.5 to 1.5
- base_head: bfloat16 [8192, 4096], P('fsdp'), may hold values from -1 to 1
- first_dir: bfloat16 [8192, 4096], P('fsdp'), may hold values from -0.09375 to 0.09375
- second_dir: bfloat16 [8192, 4096], P('fsdp'), may hold values from -0.09375 to 0.09375
- coords: int32 [8, 2], P('grid'), parts along dimension 0, may hold values from 0 to 7
- targets: int32 [512], replicated, may hold values from 0 to 8191
Outputs:
- token_loss: float32 [8, 512], P('grid', 'fsdp'), parts along dimension 0
- mean_loss: float32 [8], P('grid'), parts along dimension 0
The draws below stay inside these ranges and needn't reach their ends.
There are 4 independent parts, one for each index of `grid`. The reference program is written for one: setup_inputs(seed, part) draws one part's arguments, and reference() takes and returns one part's arrays. A program takes and returns all parts, laid end to end along the dimension named above; an argument that names none is the same for every part. Nothing has to cross between parts.
All inputs are finite; a program needn't handle non-finite values.
Results may differ from the reference program's by a relative error of at most 0.0003.
Values may be sent and summed in bfloat16 or wider, within the bound.
No kernel may reach another device: no remote copies, remote signals or barrier semaphores. Data moves between devices by JAX's collectives and lax.ppermute only.
A program may use at most 128 MiB of HBM per device.

```python
import math
import jax
import jax.numpy as jnp
from jax import lax

D = 4096
V_DEV = 1024
PTS = 2
TOKENS = 512
VOCAB = 8192
N_FSDP = 8


def spike_plan(key):
    spike_key = jax.random.fold_in(key, 7177)
    spike_rows = jax.random.randint(jax.random.fold_in(spike_key, 1), (N_FSDP,), 0, TOKENS)
    offsets = jax.random.randint(jax.random.fold_in(spike_key, 2), (N_FSDP,), 0, V_DEV)
    spike_cols = jnp.arange(N_FSDP, dtype=jnp.int32) * V_DEV + offsets
    pattern = jnp.clip(jax.random.normal(jax.random.fold_in(spike_key, 3), (N_FSDP, D), jnp.float32), -3.0, 3.0)
    return (spike_rows, spike_cols, pattern)


def draw_hidden(key, part):
    rows_all = jnp.clip(jax.random.normal(jax.random.fold_in(key, 21), (TOKENS, D), jnp.float32), -4.0, 4.0)
    spike_rows, spike_cols, pattern = spike_plan(key)
    rows_all = rows_all.at[spike_rows].set(pattern)
    return rows_all.astype(jnp.bfloat16)


def draw_base_head(key, part):
    weight = jnp.clip(jax.random.normal(jax.random.fold_in(key, 11), (VOCAB, D), jnp.float32) / math.sqrt(D), -0.25, 0.25)
    spike_rows, spike_cols, pattern = spike_plan(key)
    weight = weight.at[spike_cols].set(240.0 / D * pattern)
    return weight.astype(jnp.bfloat16)


def touch_ends(result, key, low, high):
    longest = result.shape.index(max(result.shape))
    spots = []
    for shift in (0, 1):
        where = [jax.random.randint(jax.random.fold_in(key, axis), (), 0, length) for axis, length in enumerate(result.shape)]
        where[longest] = (where[longest] + shift) % result.shape[longest]
        spots.append(tuple(where))
    return result.at[spots[0]].set(low).at[spots[1]].set(high)


def block_levels(own_key, shape, pieces, low, top_value):
    loudness = 1.0
    for dim, blocks in pieces:
        draws = jax.random.uniform(jax.random.fold_in(jax.random.fold_in(own_key, 6), dim), (blocks,), jnp.float32, low / len(pieces), top_value / len(pieces))
        loudness = loudness * jnp.repeat(jnp.exp(draws), shape[dim] // blocks).reshape((-1,) + (1,) * (len(shape) - 1 - dim))
    return loudness


def bell_draw(own_key, extent, spread, bound, cuts=(), kind=jnp.bfloat16):
    entries = spread * jax.random.normal(own_key, extent, jnp.float32)
    if cuts:
        entries = entries * block_levels(own_key, extent, cuts, -0.22, 0.18)
    return jnp.clip(entries, -bound, bound).astype(kind)


def setup_inputs(seed: int = 0, part: int = 0) -> dict:
    keys = jax.random.split(jax.random.key(seed), 8)
    own_keys = jax.random.split(jax.random.fold_in(keys[7], part), 8)
    hidden = draw_hidden(jax.random.fold_in(keys[7], 71), part)
    norm_gain = jnp.clip(1.0 + 0.1 * jax.random.normal(keys[1], (D,), jnp.float32), 0.5, 1.5)
    base_head = draw_base_head(jax.random.fold_in(keys[7], 71), part)
    first_dir = bell_draw(keys[3], (VOCAB, D), D ** -0.5, 0.09375, ((0, 8),))
    second_dir = bell_draw(keys[4], (VOCAB, D), D ** -0.5, 0.09375, ((0, 8),))
    coords = touch_ends(jax.random.randint(own_keys[5], (PTS, 2), 0, 8), jax.random.fold_in(own_keys[5], 1), 0, 7).astype(jnp.int32)
    targets = touch_ends(jax.random.randint(keys[6], (TOKENS,), 0, VOCAB), jax.random.fold_in(keys[6], 1), 0, VOCAB - 1).astype(jnp.int32)
    return dict(hidden=hidden, norm_gain=norm_gain, base_head=base_head, first_dir=first_dir, second_dir=second_dir, coords=coords, targets=targets)


epsilon = 1e-05

def reference(hidden, norm_gain, base_head, first_dir, second_dir, coords, targets):
    level_table = (2.0 * jnp.arange(8, dtype=jnp.float32) - 7.0) / 7.0
    mixing = level_table[coords]
    widened = hidden.astype(jnp.float32)
    inv_rms = lax.rsqrt(lax.optimization_barrier(jnp.mean(widened * widened, axis=1, keepdims=True)) + epsilon)
    normed = (widened * inv_rms * norm_gain).astype(jnp.bfloat16)
    losses = []
    for point_idx in range(PTS):
        head_now = (base_head.astype(jnp.float32) + mixing[point_idx, 0] * first_dir.astype(jnp.float32) + mixing[point_idx, 1] * second_dir.astype(jnp.float32)).astype(jnp.bfloat16)
        logits = jnp.dot(normed, head_now.T, preferred_element_type=jnp.float32)
        row_top = lax.optimization_barrier(jnp.max(logits, axis=1, keepdims=True))
        log_total = row_top[:, 0] + jnp.log(lax.optimization_barrier(jnp.sum(jnp.exp(logits - row_top), axis=1)))
        picked = jnp.take_along_axis(logits, targets[:, None].astype(jnp.int32), axis=1)[:, 0]
        losses.append(log_total - picked)
    token_loss = jnp.stack(losses)
    return (token_loss, lax.optimization_barrier(jnp.mean(token_loss, axis=1)))
```

```python
import jax
import jax.numpy as jnp
from jax import lax
from jax.sharding import PartitionSpec as P

epsilon = 1e-05


def mixing_of(coords):
    levels = jnp.arange(8, dtype=jnp.int32)
    level_table = (2.0 * levels.astype(jnp.float32) - 7.0) / 7.0
    chosen = (coords[:, :, None] == levels[None, None, :]).astype(jnp.float32)
    return jnp.sum(chosen * level_table, axis=2)


def swap(a, axis, mask):
    return lax.ppermute(a, axis, [(i, i ^ mask) for i in range(lax.axis_size(axis))])


def body(hidden, norm_gain, base_head, first_dir, second_dir, coords, targets):
    n_grid, n_fsdp = lax.axis_size("grid"), lax.axis_size("fsdp")
    grid_idx, shard_idx = lax.axis_index("grid"), lax.axis_index("fsdp")
    own_count = hidden.shape[0]
    sub = own_count // n_grid
    pts = coords.shape[0]
    vocab_count = base_head.shape[0]
    own = lax.dynamic_slice_in_dim(hidden, grid_idx * sub, sub, 0)
    slots = [None] * n_fsdp
    slots[0] = own
    for j in range(2, n_fsdp, 2):
        slots[j] = swap(own, "fsdp", j)
    for j in range(0, n_fsdp, 2):
        slots[j + 1] = swap(slots[j], "fsdp", 1)
    mine = mixing_of(coords)
    mixing = jnp.zeros((n_grid, pts, 2), jnp.float32)
    for j in range(n_grid):
        part = mine if j == 0 else swap(mine, "grid", j)
        mixing = lax.dynamic_update_index_in_dim(mixing, part, grid_idx ^ j, 0)
    mixing = mixing.reshape(n_grid * pts, 2)

    widened = jnp.stack(slots).reshape(n_fsdp * sub, -1).astype(jnp.float32)
    inv_rms = lax.rsqrt(jnp.mean(widened * widened, axis=1, keepdims=True) + epsilon)
    normed = (widened * inv_rms * norm_gain).astype(jnp.bfloat16)
    dots = [
        jnp.einsum("td,vd->tv", normed, w, preferred_element_type=jnp.float32)
        for w in (base_head, first_dir, second_dir)
    ]
    order = shard_idx ^ jnp.arange(n_fsdp, dtype=jnp.int32)
    group_targets = lax.dynamic_index_in_dim(targets.reshape(n_fsdp, n_grid, sub), grid_idx, 1, False)
    target_col = jnp.take(group_targets, order, axis=0).reshape(-1) - shard_idx * vocab_count
    matches = target_col[:, None] == jnp.arange(vocab_count, dtype=jnp.int32)[None, :]
    stats = []
    for p in range(n_grid * pts):
        logits = dots[0] + mixing[p, 0] * dots[1] + mixing[p, 1] * dots[2]
        top = jnp.max(logits, axis=1)
        total = jnp.sum(jnp.exp(logits - top[:, None]), axis=1)
        picked = jnp.sum(jnp.where(matches, logits, 0.0), axis=1)
        stats.append(jnp.stack([top + jnp.log(total), picked]))
    stats = jnp.stack(stats).reshape(n_grid, pts, 2, n_fsdp, sub)
    stats = jnp.take(stats, order, axis=3)
    sent = jnp.broadcast_to(stats[:, None], (n_grid, n_fsdp) + stats.shape[1:])
    sent = sent.reshape((n_grid * n_fsdp,) + stats.shape[1:])
    got = lax.all_to_all(sent, ("grid", "fsdp"), 0, 0)
    got = got.reshape(n_grid, n_fsdp, pts, 2, n_fsdp, sub)
    part_lse = got[:, :, :, 0]
    row_top = jnp.max(part_lse, axis=1)
    lse = row_top + jnp.log(jnp.sum(jnp.exp(part_lse - row_top[:, None]), axis=1))
    loss = lse - jnp.sum(got[:, :, :, 1], axis=1)
    mean_loss = jnp.mean(loss, axis=(0, 2, 3))
    token_loss = lax.dynamic_index_in_dim(loss, shard_idx, 2, False)
    token_loss = token_loss.transpose(1, 0, 2).reshape(pts, own_count)
    return (token_loss, mean_loss)


def solution(mesh):
    placed = (
        P("fsdp", None),
        P(),
        P("fsdp", None),
        P("fsdp", None),
        P("fsdp", None),
        P("grid", None),
        P(),
    )
    return jax.shard_map(
        body, mesh=mesh, in_specs=placed, out_specs=(P("grid", "fsdp"), P("grid")), check_vma=False
    )
```

```python
import functools
import jax
import jax.numpy as jnp
from jax import lax
from jax.experimental import pallas as pl
from jax.experimental.pallas import tpu as pltpu
from jax.sharding import PartitionSpec as P

epsilon = 1e-05


def mixing_of(coords):
    levels = jnp.arange(8, dtype=jnp.int32)
    level_table = (2.0 * levels.astype(jnp.float32) - 7.0) / 7.0
    chosen = (coords[:, :, None] == levels[None, None, :]).astype(jnp.float32)
    return jnp.sum(chosen * level_table, axis=2)


def swap(a, axis, mask):
    return lax.ppermute(a, axis, [(i, i ^ mask) for i in range(lax.axis_size(axis))])


def head_kernel(n_fsdp, n_grid, pts, shard_ref, *refs):
    mixing_refs, refs = refs[:n_grid], refs[n_grid:]
    chunks = refs[:n_fsdp]
    gain_ref, target_ref, base_ref, first_ref, second_ref, out_ref, rows_ref, dots_ref = refs[n_fsdp:]
    shard_idx = shard_ref[0]
    for j in range(n_fsdp):
        widened = chunks[j][...].astype(jnp.float32)
        inv_rms = lax.rsqrt(jnp.mean(widened * widened, axis=1, keepdims=True) + epsilon)
        rows_ref[shard_idx ^ j] = (widened * inv_rms * gain_ref[...]).astype(jnp.bfloat16)
    tokens = n_fsdp * chunks[0].shape[0]
    rows = rows_ref[...].reshape(tokens, rows_ref.shape[2])
    vocab_count = base_ref.shape[0]
    for k, weight_ref in enumerate((base_ref, first_ref, second_ref)):
        dots_ref[k] = lax.dot_general(
            rows, weight_ref[...], (((1,), (1,)), ((), ())), preferred_element_type=jnp.float32
        )
    columns = lax.broadcasted_iota(jnp.int32, (tokens, vocab_count), 1) + shard_idx * vocab_count
    matches = columns == target_ref[...]
    found = [
        jnp.sum(jnp.where(matches, dots_ref[k], 0.0), axis=1, keepdims=True) for k in range(3)
    ]
    lane = lax.broadcasted_iota(jnp.int32, (tokens, 128), 1)
    table = jnp.zeros((tokens, 128), jnp.float32)
    for p in range(n_grid * pts):
        mixing_ref, point = mixing_refs[p // pts], p % pts
        a, b = mixing_ref[point, 0], mixing_ref[point, 1]
        logits = dots_ref[0] + a * dots_ref[1] + b * dots_ref[2]
        top = jnp.max(logits, axis=1, keepdims=True)
        total = jnp.sum(jnp.exp(logits - top), axis=1, keepdims=True)
        row = (shard_ref[1] ^ (p // pts)) * 2 * pts + point
        table = jnp.where(lane == row, top + jnp.log(total), table)
        table = jnp.where(lane == row + pts, found[0] + a * found[1] + b * found[2], table)
    flipped = table.T
    for g in range(n_grid):
        block = flipped[g * 2 * pts : (g + 1) * 2 * pts]
        for f in range(n_fsdp):
            out_ref[g, f] = block


def load_kernel(shard_ref, rows_ref, mixing_ref, target_ref, *refs):
    count = (len(refs) - 1) // 2
    copies = [
        pltpu.make_async_copy(refs[k], refs[count + k], refs[-1].at[k]) for k in range(count)
    ]
    for copy in copies:
        copy.start()
    for copy in copies:
        copy.wait()


def loss_kernel(sub, shard_ref, got_ref, token_ref, mean_ref):
    n_grid, n_fsdp, _, tokens = got_ref.shape
    pts = token_ref.shape[0]
    shift = (n_fsdp - shard_ref[0]) * sub
    sums = jnp.zeros((pts, tokens), jnp.float32)
    for g in range(n_grid):
        parts = [got_ref[g, f] for f in range(n_fsdp)]
        top = functools.reduce(jnp.maximum, parts)
        total = sum(jnp.exp(part - top) for part in parts)
        lse = (top + jnp.log(total))[:pts]
        loss = lse - sum(parts)[pts:]
        sums = sums + loss
        token_ref[:, g * sub : (g + 1) * sub] = pltpu.roll(loss, shift, 1)[:, :sub]
    mean_ref[...] = jnp.sum(sums, axis=1, keepdims=True) / (n_grid * tokens)


def body(hidden, norm_gain, base_head, first_dir, second_dir, coords, targets):
    n_grid, n_fsdp = lax.axis_size("grid"), lax.axis_size("fsdp")
    grid_idx, shard_idx = lax.axis_index("grid"), lax.axis_index("fsdp")
    own_count, width = hidden.shape
    sub = own_count // n_grid
    tokens = n_fsdp * sub
    pts = coords.shape[0]
    vocab_count = base_head.shape[0]
    own = lax.dynamic_slice_in_dim(hidden, grid_idx * sub, sub, 0)
    slots = [None] * n_fsdp
    slots[0] = own
    for j in range(2, n_fsdp, 2):
        slots[j] = swap(own, "fsdp", j)
    for j in range(0, n_fsdp, 2):
        slots[j + 1] = swap(slots[j], "fsdp", 1)
    mine = mixing_of(coords)
    mixing = [mine]
    for j in range(1, n_grid):
        mixing.append(swap(mine, "grid", j))
    group_targets = lax.dynamic_index_in_dim(targets.reshape(n_fsdp, n_grid, sub), grid_idx, 1, False)
    group_targets = group_targets.reshape(tokens, 1)
    shard = jnp.stack([shard_idx, grid_idx]).astype(jnp.int32)

    smem = pl.BlockSpec(memory_space=pltpu.SMEM)
    vmem = pl.BlockSpec(memory_space=pltpu.VMEM)
    heads = [
        pltpu.with_memory_space_constraint(w, pltpu.HBM) for w in (base_head, first_dir, second_dir)
    ]
    anywhere = pl.BlockSpec(memory_space=pltpu.HBM)
    weights = pl.pallas_call(
        load_kernel,
        out_shape=tuple(pltpu.VMEM(w.shape, w.dtype) for w in heads),
        in_specs=[pl.BlockSpec(memory_space=pl.ANY)] * 4 + [anywhere] * 3,
        out_specs=(vmem,) * 3,
        scratch_shapes=[pltpu.SemaphoreType.DMA((3,))],
        compiler_params=pltpu.CompilerParams(vmem_limit_bytes=1024 * 1024),
        cost_estimate=pl.CostEstimate(flops=LOAD_FLOPS, transcendentals=0, bytes_accessed=6 * base_head.size),
        name="load_heads",
    )(shard, own, mine, group_targets, *heads)
    sent = pl.pallas_call(
        functools.partial(head_kernel, n_fsdp, n_grid, pts),
        out_shape=jax.ShapeDtypeStruct((n_grid, n_fsdp, 2 * pts, tokens), jnp.float32),
        in_specs=[smem] * (1 + n_grid) + [vmem] * (n_fsdp + 5),
        out_specs=vmem,
        scratch_shapes=[
            pltpu.VMEM((n_fsdp, sub, width), jnp.bfloat16),
            pltpu.VMEM((3, tokens, vocab_count), jnp.float32),
        ],
        compiler_params=pltpu.CompilerParams(vmem_limit_bytes=VMEM_LIMIT),
        name="head_stats",
    )(shard, *mixing, *slots, norm_gain.reshape(1, width), group_targets, *weights)
    got = lax.all_to_all(
        sent.reshape(n_grid * n_fsdp, 2 * pts, tokens), ("grid", "fsdp"), 0, 0
    ).reshape(n_grid, n_fsdp, 2 * pts, tokens)
    token_loss, mean_loss = pl.pallas_call(
        functools.partial(loss_kernel, sub),
        out_shape=(
            jax.ShapeDtypeStruct((pts, own_count), jnp.float32),
            jax.ShapeDtypeStruct((pts, 1), jnp.float32),
        ),
        in_specs=[smem, vmem],
        out_specs=(vmem, vmem),
        compiler_params=pltpu.CompilerParams(vmem_limit_bytes=4 * 1024 * 1024),
        name="loss_join",
    )(shard, got)
    return (token_loss, mean_loss.reshape(pts))


LOAD_FLOPS = 40_000_000
VMEM_LIMIT = 16 * 1024 * 1024


def solution(mesh):
    placed = (
        P("fsdp", None),
        P(),
        P("fsdp", None),
        P("fsdp", None),
        P("fsdp", None),
        P("grid", None),
        P(),
    )
    return jax.shard_map(
        body, mesh=mesh, in_specs=placed, out_specs=(P("grid", "fsdp"), P("grid")), check_vma=False
    )
```

```python
import functools
import math
import jax
import jax.numpy as jnp
from jax import lax
from jax.experimental import pallas as pl
from jax.experimental.pallas import tpu as pltpu
from jax.sharding import PartitionSpec as P

epsilon = 1e-05


def swap(a, axis, mask):
    return lax.ppermute(a, axis, [(i, i ^ mask) for i in range(lax.axis_size(axis))])


def head_kernel(n_fsdp, n_grid, pts, shard_ref, *refs):
    coords_refs, refs = refs[:n_grid], refs[n_grid:]
    chunks, refs = refs[:n_fsdp], refs[n_fsdp:]
    gain_ref, target_ref, base_ref, first_ref, second_hbm, out_ref = refs[:6]
    rows_ref, second_ref, dots_ref, arrived = refs[6:]
    fetch = pltpu.make_async_copy(second_hbm, second_ref, arrived)
    fetch.start()
    shard_idx, grid_idx = shard_ref[0], shard_ref[1]
    for j in range(n_fsdp):
        widened = chunks[j][...].astype(jnp.float32)
        inv_rms = lax.rsqrt(jnp.mean(widened * widened, axis=1, keepdims=True) + epsilon)
        rows_ref[shard_idx ^ j] = (widened * inv_rms * gain_ref[...]).astype(jnp.bfloat16)
    tokens = n_fsdp * chunks[0].shape[0]
    rows = rows_ref[...].reshape(tokens, rows_ref.shape[2])
    vocab_count = base_ref.shape[0]
    block = math.gcd(vocab_count, 256)

    def dot_of(weight):
        return lax.dot_general(
            weight, rows, (((1,), (1,)), ((), ())), preferred_element_type=jnp.float32
        )

    dots_ref[0] = dot_of(base_ref[...])
    dots_ref[1] = dot_of(first_ref[...])
    fetch.wait()
    points = []
    for j in range(n_grid):
        for p in range(pts):
            level = [jnp.full((8, tokens), coords_refs[j][p, k], jnp.int32) for k in range(2)]
            points.append([(2.0 * c.astype(jnp.float32) - 7.0) / 7.0 for c in level])
    state = [None] * len(points)
    found = [jnp.zeros((8, tokens), jnp.float32)] * 3
    row_of = 8 * lax.broadcasted_iota(jnp.int32, (block // 8, 8, tokens), 0)
    row_of = row_of + lax.broadcasted_iota(jnp.int32, (block // 8, 8, tokens), 1)
    wanted = target_ref[...] - shard_idx * vocab_count
    for start in range(0, vocab_count, block):
        span = pl.ds(start, block)
        parts = [dots_ref[0, span], dots_ref[1, span], dot_of(second_ref[span])]
        parts = [part.reshape(block // 8, 8, tokens) for part in parts]
        matches = row_of == (wanted - start)[None]
        found = [
            old + jnp.sum(jnp.where(matches, part, 0.0), axis=0) for old, part in zip(found, parts)
        ]
        for n, (a, b) in enumerate(points):
            logits = parts[0] + a[None] * parts[1] + b[None] * parts[2]
            top = jnp.max(logits, axis=0)
            if state[n] is not None:
                top = jnp.maximum(top, state[n][0])
            total = jnp.sum(jnp.exp(logits - top[None]), axis=0)
            if state[n] is not None:
                total = total + state[n][1] * jnp.exp(state[n][0] - top)
            state[n] = (top, total)
    for j in range(n_grid):
        lines = [[], []]
        for p in range(pts):
            (a, b), (tops, totals) = points[j * pts + p], state[j * pts + p]
            top = jnp.max(tops, axis=0, keepdims=True)
            total = jnp.sum(totals * jnp.exp(tops - top), axis=0, keepdims=True)
            lines[0].append(top + jnp.log(total))
            picked = found[0] + a * found[1] + b * found[2]
            lines[1].append(jnp.sum(picked, axis=0, keepdims=True))
        packed = jnp.concatenate(lines[0] + lines[1], axis=0)
        for f in range(n_fsdp):
            out_ref[grid_idx ^ j, f] = packed


def load_kernel(shard_ref, rows_ref, target_ref, *refs):
    count = (len(refs) - 1) // 2
    copies = [
        pltpu.make_async_copy(refs[k], refs[count + k], refs[-1].at[k]) for k in range(count)
    ]
    for copy in copies:
        copy.start()
    for copy in copies:
        copy.wait()


def loss_kernel(sub, shard_ref, got_ref, token_ref, mean_ref):
    n_grid, n_fsdp, _, tokens = got_ref.shape
    pts = token_ref.shape[0]
    shift = (n_fsdp - shard_ref[0]) * sub
    sums = jnp.zeros((pts, tokens), jnp.float32)
    for g in range(n_grid):
        parts = [got_ref[g, f] for f in range(n_fsdp)]
        top = functools.reduce(jnp.maximum, parts)
        total = sum(jnp.exp(part - top) for part in parts)
        lse = (top + jnp.log(total))[:pts]
        loss = lse - sum(parts)[pts:]
        sums = sums + loss
        token_ref[:, g * sub : (g + 1) * sub] = pltpu.roll(loss, shift, 1)[:, :sub]
    for p in range(pts):
        mean_ref[p] = jnp.sum(sums[p : p + 1]) / (n_grid * tokens)


def body(hidden, norm_gain, base_head, first_dir, second_dir, coords, targets):
    n_grid, n_fsdp = lax.axis_size("grid"), lax.axis_size("fsdp")
    grid_idx, shard_idx = lax.axis_index("grid"), lax.axis_index("fsdp")
    own_count, width = hidden.shape
    sub = own_count // n_grid
    tokens = n_fsdp * sub
    pts = coords.shape[0]
    vocab_count = base_head.shape[0]
    own = lax.dynamic_slice_in_dim(hidden, grid_idx * sub, sub, 0)
    slots = [None] * n_fsdp
    slots[0] = own
    for j in range(2, n_fsdp, 2):
        slots[j] = swap(own, "fsdp", j)
    for j in range(0, n_fsdp, 2):
        slots[j + 1] = swap(slots[j], "fsdp", 1)
    mixing = [coords]
    for j in range(1, n_grid):
        mixing.append(swap(coords, "grid", j))
    group_targets = lax.dynamic_index_in_dim(targets.reshape(n_fsdp, n_grid, sub), grid_idx, 1, False)
    group_targets = group_targets.reshape(1, tokens)
    shard = jnp.stack([shard_idx, grid_idx]).astype(jnp.int32)

    smem = pl.BlockSpec(memory_space=pltpu.SMEM)
    vmem = pl.BlockSpec(memory_space=pltpu.VMEM)
    heads = [
        pltpu.with_memory_space_constraint(w, pltpu.HBM) for w in (base_head, first_dir)
    ]
    anywhere = pl.BlockSpec(memory_space=pltpu.HBM)
    weights = pl.pallas_call(
        load_kernel,
        out_shape=tuple(pltpu.VMEM(w.shape, w.dtype) for w in heads),
        in_specs=[pl.BlockSpec(memory_space=pl.ANY)] * 3 + [anywhere] * 2,
        out_specs=(vmem,) * 2,
        scratch_shapes=[pltpu.SemaphoreType.DMA((2,))],
        compiler_params=pltpu.CompilerParams(vmem_limit_bytes=1024 * 1024),
        cost_estimate=pl.CostEstimate(flops=LOAD_FLOPS, transcendentals=0, bytes_accessed=4 * base_head.size),
        name="load_heads",
    )(shard, own, group_targets, *heads)
    sent = pl.pallas_call(
        functools.partial(head_kernel, n_fsdp, n_grid, pts),
        out_shape=jax.ShapeDtypeStruct((n_grid, n_fsdp, 2 * pts, tokens), jnp.float32),
        in_specs=[smem] * (1 + n_grid) + [vmem] * (n_fsdp + 4) + [anywhere],
        out_specs=vmem,
        scratch_shapes=[
            pltpu.VMEM((n_fsdp, sub, width), jnp.bfloat16),
            pltpu.VMEM(second_dir.shape, second_dir.dtype),
            pltpu.VMEM((2, vocab_count, tokens), jnp.float32),
            pltpu.SemaphoreType.DMA,
        ],
        compiler_params=pltpu.CompilerParams(vmem_limit_bytes=VMEM_LIMIT),
        name="head_stats",
    )(shard, *mixing, *slots, norm_gain.reshape(1, width), group_targets, *weights, pltpu.with_memory_space_constraint(second_dir, pltpu.HBM))
    got = lax.all_to_all(
        sent.reshape(n_grid * n_fsdp, 2 * pts, tokens), ("grid", "fsdp"), 0, 0
    ).reshape(n_grid, n_fsdp, 2 * pts, tokens)
    token_loss, mean_loss = pl.pallas_call(
        functools.partial(loss_kernel, sub),
        out_shape=(
            jax.ShapeDtypeStruct((pts, own_count), jnp.float32),
            jax.ShapeDtypeStruct((pts,), jnp.float32),
        ),
        in_specs=[smem, vmem],
        out_specs=(vmem, smem),
        compiler_params=pltpu.CompilerParams(vmem_limit_bytes=4 * 1024 * 1024),
        name="loss_join",
    )(shard, got)
    return (token_loss, mean_loss)


LOAD_FLOPS = 40_000_000
VMEM_LIMIT = 16 * 1024 * 1024


def solution(mesh):
    placed = (
        P("fsdp", None),
        P(),
        P("fsdp", None),
        P("fsdp", None),
        P("fsdp", None),
        P("grid", None),
        P(),
    )
    return jax.shard_map(
        body, mesh=mesh, in_specs=placed, out_specs=(P("grid", "fsdp"), P("grid")), check_vma=False
    )
```

```python
import functools
import math
import jax
import jax.numpy as jnp
from jax import lax
from jax.experimental import pallas as pl
from jax.experimental.pallas import tpu as pltpu
from jax.sharding import PartitionSpec as P

epsilon = 1e-05


def swap(a, axis, mask):
    return lax.ppermute(a, axis, [(i, i ^ mask) for i in range(lax.axis_size(axis))])


def head_kernel(n_fsdp, n_grid, pts, shard_ref, *refs):
    coords_refs, refs = refs[:n_grid], refs[n_grid:]
    chunks, refs = refs[:n_fsdp], refs[n_fsdp:]
    gain_ref, target_ref, base_ref, first_ref, second_ref, out_ref = refs[:6]
    rows_ref, dots_ref = refs[6:]
    shard_idx, grid_idx = shard_ref[0], shard_ref[1]
    for j in range(n_fsdp):
        widened = chunks[j][...].astype(jnp.float32)
        inv_rms = lax.rsqrt(jnp.mean(widened * widened, axis=1, keepdims=True) + epsilon)
        rows_ref[shard_idx ^ j] = (widened * inv_rms * gain_ref[...]).astype(jnp.bfloat16)
    tokens = n_fsdp * chunks[0].shape[0]
    rows = rows_ref[...].reshape(tokens, rows_ref.shape[2])
    vocab_count = base_ref.shape[0]
    block = math.gcd(vocab_count, 256)

    def dot_of(weight):
        return lax.dot_general(
            weight, rows, (((1,), (1,)), ((), ())), preferred_element_type=jnp.float32
        )

    dots_ref[0] = dot_of(base_ref[...])
    dots_ref[1] = dot_of(first_ref[...])
    points = []
    for j in range(n_grid):
        for p in range(pts):
            level = [jnp.full((8, tokens), coords_refs[j][p, k], jnp.int32) for k in range(2)]
            points.append([(2.0 * c.astype(jnp.float32) - 7.0) / 7.0 for c in level])
    state = [None] * len(points)
    found = [jnp.zeros((8, tokens), jnp.float32)] * 3
    row_of = 8 * lax.broadcasted_iota(jnp.int32, (block // 8, 8, tokens), 0)
    row_of = row_of + lax.broadcasted_iota(jnp.int32, (block // 8, 8, tokens), 1)
    wanted = target_ref[...] - shard_idx * vocab_count
    for start in range(0, vocab_count, block):
        span = pl.ds(start, block)
        parts = [dots_ref[0, span], dots_ref[1, span], dot_of(second_ref[span])]
        parts = [part.reshape(block // 8, 8, tokens) for part in parts]
        matches = row_of == (wanted - start)[None]
        found = [
            old + jnp.sum(jnp.where(matches, part, 0.0), axis=0) for old, part in zip(found, parts)
        ]
        for n, (a, b) in enumerate(points):
            logits = parts[0] + a[None] * parts[1] + b[None] * parts[2]
            top = jnp.max(logits, axis=0)
            if state[n] is not None:
                top = jnp.maximum(top, state[n][0])
            total = jnp.sum(jnp.exp(logits - top[None]), axis=0)
            if state[n] is not None:
                total = total + state[n][1] * jnp.exp(state[n][0] - top)
            state[n] = (top, total)
    for j in range(n_grid):
        lines = [[], []]
        for p in range(pts):
            (a, b), (tops, totals) = points[j * pts + p], state[j * pts + p]
            top = jnp.max(tops, axis=0, keepdims=True)
            total = jnp.sum(totals * jnp.exp(tops - top), axis=0, keepdims=True)
            lines[0].append(top + jnp.log(total))
            picked = found[0] + a * found[1] + b * found[2]
            lines[1].append(jnp.sum(picked, axis=0, keepdims=True))
        packed = jnp.concatenate(lines[0] + lines[1], axis=0)
        for f in range(n_fsdp):
            out_ref[grid_idx ^ j, f] = packed


def copies_of(pairs, arrived):
    copies = []
    for source, target in pairs:
        count = source.shape[0] // PIECES
        for piece in range(PIECES):
            span = pl.ds(piece * count, count)
            copies.append(
                pltpu.make_async_copy(source.at[span], target.at[span], arrived.at[len(copies)])
            )
    return copies


def load_kernel(shard_ref, rows_ref, target_ref, *refs):
    count = (len(refs) - 1) // 2
    copies = copies_of(list(zip(refs[:count], refs[count : 2 * count])), refs[-1])
    for copy in copies:
        copy.start()
    for copy in copies:
        copy.wait()


def loss_kernel(sub, shard_ref, got_ref, token_ref, mean_ref):
    n_grid, n_fsdp, _, tokens = got_ref.shape
    pts = token_ref.shape[0]
    shift = (n_fsdp - shard_ref[0]) * sub
    sums = jnp.zeros((pts, tokens), jnp.float32)
    for g in range(n_grid):
        parts = [got_ref[g, f] for f in range(n_fsdp)]
        top = functools.reduce(jnp.maximum, parts)
        total = sum(jnp.exp(part - top) for part in parts)
        lse = (top + jnp.log(total))[:pts]
        loss = lse - sum(parts)[pts:]
        sums = sums + loss
        token_ref[:, g * sub : (g + 1) * sub] = pltpu.roll(loss, shift, 1)[:, :sub]
    for p in range(pts):
        mean_ref[p] = jnp.sum(sums[p : p + 1]) / (n_grid * tokens)


def body(hidden, norm_gain, base_head, first_dir, second_dir, coords, targets):
    n_grid, n_fsdp = lax.axis_size("grid"), lax.axis_size("fsdp")
    grid_idx, shard_idx = lax.axis_index("grid"), lax.axis_index("fsdp")
    own_count, width = hidden.shape
    sub = own_count // n_grid
    tokens = n_fsdp * sub
    pts = coords.shape[0]
    vocab_count = base_head.shape[0]
    own = lax.dynamic_slice_in_dim(hidden, grid_idx * sub, sub, 0)
    slots = [None] * n_fsdp
    slots[0] = own
    for j in range(2, n_fsdp, 2):
        slots[j] = swap(own, "fsdp", j)
    for j in range(0, n_fsdp, 2):
        slots[j + 1] = swap(slots[j], "fsdp", 1)
    mixing = [coords]
    for j in range(1, n_grid):
        mixing.append(swap(coords, "grid", j))
    group_targets = lax.dynamic_index_in_dim(targets.reshape(n_fsdp, n_grid, sub), grid_idx, 1, False)
    group_targets = group_targets.reshape(1, tokens)
    shard = jnp.stack([shard_idx, grid_idx]).astype(jnp.int32)

    smem = pl.BlockSpec(memory_space=pltpu.SMEM)
    vmem = pl.BlockSpec(memory_space=pltpu.VMEM)
    heads = [
        pltpu.with_memory_space_constraint(w, pltpu.HBM) for w in (base_head, first_dir, second_dir)
    ]
    anywhere = pl.BlockSpec(memory_space=pltpu.HBM)
    weights = pl.pallas_call(
        load_kernel,
        out_shape=tuple(pltpu.VMEM(w.shape, w.dtype) for w in heads),
        in_specs=[pl.BlockSpec(memory_space=pl.ANY)] * 3 + [anywhere] * 3,
        out_specs=(vmem,) * 3,
        scratch_shapes=[pltpu.SemaphoreType.DMA((3 * PIECES,))],
        compiler_params=pltpu.CompilerParams(vmem_limit_bytes=1024 * 1024),
        cost_estimate=pl.CostEstimate(flops=LOAD_FLOPS, transcendentals=0, bytes_accessed=4 * base_head.size),
        name="load_heads",
    )(shard, own, group_targets, *heads)
    sent = pl.pallas_call(
        functools.partial(head_kernel, n_fsdp, n_grid, pts),
        out_shape=jax.ShapeDtypeStruct((n_grid, n_fsdp, 2 * pts, tokens), jnp.float32),
        in_specs=[smem] * (1 + n_grid) + [vmem] * (n_fsdp + 5),
        out_specs=vmem,
        scratch_shapes=[
            pltpu.VMEM((n_fsdp, sub, width), jnp.bfloat16),
            pltpu.VMEM((2, vocab_count, tokens), jnp.float32),
        ],
        compiler_params=pltpu.CompilerParams(vmem_limit_bytes=VMEM_LIMIT),
        name="head_stats",
    )(shard, *mixing, *slots, norm_gain.reshape(1, width), group_targets, *weights)
    got = lax.all_to_all(
        sent.reshape(n_grid * n_fsdp, 2 * pts, tokens), ("grid", "fsdp"), 0, 0
    ).reshape(n_grid, n_fsdp, 2 * pts, tokens)
    token_loss, mean_loss = pl.pallas_call(
        functools.partial(loss_kernel, sub),
        out_shape=(
            jax.ShapeDtypeStruct((pts, own_count), jnp.float32),
            jax.ShapeDtypeStruct((pts,), jnp.float32),
        ),
        in_specs=[smem, vmem],
        out_specs=(vmem, smem),
        compiler_params=pltpu.CompilerParams(vmem_limit_bytes=4 * 1024 * 1024),
        name="loss_join",
    )(shard, got)
    return (token_loss, mean_loss)


LOAD_FLOPS = 40_000_000
PIECES = 4
VMEM_LIMIT = 16 * 1024 * 1024


def solution(mesh):
    placed = (
        P("fsdp", None),
        P(),
        P("fsdp", None),
        P("fsdp", None),
        P("fsdp", None),
        P("grid", None),
        P(),
    )
    return jax.shard_map(
        body, mesh=mesh, in_specs=placed, out_specs=(P("grid", "fsdp"), P("grid")), check_vma=False
    )
```
